32 devices in a mesh: row: 4 (over x, core), col: 8 (over z, y).
Axes of the slice: x: 2, y: 2, z: 4, core: 2. Of those that a mesh axis runs over, the one named last changes fastest.
Arguments:
- train_docs: bfloat16 [32768, 768], P(('row', 'col')), may hold values from -85 to 85
- eval_rows: bfloat16 [2048, 768], P(('row', 'col')), may hold values from -85 to 85
- bench_ids: int32 [2048, 1], P(('row', 'col')), may hold values from 0 to 127
Outputs:
- row_best: float32 [32768], P(('row', 'col'))
- bench_best: float32 [128], replicated
The draws below stay inside these ranges and needn't reach their ends.
Inputs may be any that keep to these rules, and one draw needn't show every extreme that they name: `bench_ids`: every benchmark has at least one question.
All inputs are finite; a program needn't handle non-finite values.
Results may differ from the reference program's by a relative error of at most 0.0003.
Values may be sent and summed in bfloat16 or wider, within the bound.
A program may use at most 64 MiB of HBM per device.

```python
import math
import jax
import jax.numpy as jnp
from jax import lax

D = 768
NBENCH = 128
EVAL = 2048
TRAIN = 32768


def base_train(key):
    return jnp.clip(jax.random.normal(jax.random.fold_in(key, 11), (TRAIN, D), jnp.float32), -6.0, 6.0)


def draw_train_docs(key, part):
    rows_out = base_train(key)
    return rows_out.astype(jnp.bfloat16)


def draw_eval_rows(key, part):
    trained = base_train(key)
    fresh_rows = jnp.clip(jax.random.normal(jax.random.fold_in(key, 12), (EVAL, D), jnp.float32), -6.0, 6.0)
    picked = jax.random.randint(jax.random.fold_in(key, 13), (EVAL,), 0, TRAIN)
    flagged = jax.random.randint(jax.random.fold_in(key, 14), (EVAL,), 0, 4) == 0
    strength = jax.random.uniform(jax.random.fold_in(key, 15), (EVAL, 1), jnp.float32, 0.4, 1.0)
    copies = jnp.take(trained, picked, axis=0)
    mixed = strength * copies + jnp.sqrt(1.0 - strength * strength) * fresh_rows
    rows_out = jnp.where(flagged[:, None], mixed, fresh_rows)
    return rows_out.astype(jnp.bfloat16)


def distinct(key, rows, count, top, lift):
    sequence = jax.random.permutation(jax.random.fold_in(key, 1), count)
    favour = sequence
    for power in range(3):
        favour = favour * favour // count
    favour = favour * lift // count
    chance = jax.random.randint(jax.random.fold_in(key, 2), (rows, count), 0, 4096) + favour
    holders = jax.random.permutation(jax.random.fold_in(key, 3), rows)[jnp.arange(count) % rows]
    chance = jnp.where(jnp.arange(rows)[:, None] == holders[None, :], 1 << 14, chance)
    score = chance * count + jnp.arange(count)
    return lax.top_k(score.astype(jnp.int32), top)[1].astype(jnp.int32)


def setup_inputs(seed: int = 0) -> dict:
    key_of = jax.random.split(jax.random.key(seed), 4)
    train_docs = draw_train_docs(jax.random.fold_in(key_of[3], 71), 0)
    eval_rows = draw_eval_rows(jax.random.fold_in(key_of[3], 71), 0)
    bench_ids = distinct(key_of[2], EVAL, NBENCH, 1, 64)
    return dict(train_docs=train_docs, eval_rows=eval_rows, bench_ids=bench_ids)


epsilon = 1e-06

def scales(embedded):
    squares = lax.optimization_barrier(jnp.mean(jnp.square(embedded.astype(jnp.float32)), axis=1))
    return lax.rsqrt(squares + epsilon) / math.sqrt(embedded.shape[1])

def bench_max(column_best, labels, count):
    matches = labels[:, None] == jnp.arange(count, dtype=jnp.int32)[None, :]
    return lax.optimization_barrier(jnp.max(jnp.where(matches, column_best[:, None], -jnp.inf), axis=0))

def reference(train_docs, eval_rows, bench_ids):
    eval_scale = scales(eval_rows)
    height = math.gcd(TRAIN, 1024)
    grouped = train_docs.reshape(TRAIN // height, height, D)

    def one_block(portion):
        train_scale = scales(portion)
        products = lax.dot_general(portion, eval_rows, (((1,), (1,)), ((), ())), preferred_element_type=jnp.float32)
        scored = products * train_scale[:, None] * eval_scale[None, :]
        return (lax.optimization_barrier(jnp.max(scored, axis=1)), lax.optimization_barrier(jnp.max(scored, axis=0)))
    row_parts, column_parts = lax.map(one_block, grouped)
    row_best = row_parts.reshape(TRAIN)
    column_best = lax.optimization_barrier(jnp.max(column_parts, axis=0))
    bench_best = bench_max(column_best, bench_ids[:, 0], NBENCH)
    return (row_best, bench_best)
```

```python
import math

import jax
import jax.numpy as jnp
from jax import lax
from jax.sharding import PartitionSpec as P

NBENCH = 128


epsilon = 1e-06


def scales(embedded):
    squares = jnp.mean(jnp.square(embedded.astype(jnp.float32)), axis=1)
    return lax.rsqrt(squares + epsilon) / math.sqrt(embedded.shape[1])


def bench_max(column_best, labels, count):
    matches = labels[:, None] == jnp.arange(count, dtype=jnp.int32)[None, :]
    return jnp.max(jnp.where(matches, column_best[:, None], -jnp.inf), axis=0)


def body(train_docs, eval_rows, bench_ids):
    questions = lax.all_gather(eval_rows, ("row", "col"), axis=0, tiled=True)
    labels = lax.all_gather(bench_ids[:, 0], ("row", "col"), axis=0, tiled=True)
    products = lax.dot_general(
        train_docs, questions, (((1,), (1,)), ((), ())), preferred_element_type=jnp.float32
    )
    scored = products * scales(train_docs)[:, None] * scales(questions)[None, :]
    best_row = jnp.max(scored, axis=1)
    best_col = jnp.max(scored, axis=0)
    bench_best = lax.pmax(bench_max(best_col, labels, NBENCH), ("row", "col"))
    return (best_row, bench_best)


def solution(mesh):
    in_specs = (P(("row", "col"), None), P(("row", "col"), None), P(("row", "col"), None))
    out_specs = (P(("row", "col")), P())
    return jax.shard_map(body, mesh=mesh, in_specs=in_specs, out_specs=out_specs, check_vma=False)
```

```python
import functools
import math

import jax
import jax.numpy as jnp
from jax import lax
from jax.experimental import pallas as pl
from jax.experimental.pallas import tpu as pltpu
from jax.sharding import PartitionSpec as P

NBENCH = 128
CORES = 2
PARTS = 4
TILE = 256
LANES = 128

epsilon = 1e-06
MESH = pl.DeviceIdType.MESH


def fold_lanes(values, op):
    total = values[:, :LANES]
    for start in range(LANES, values.shape[1], LANES):
        total = op(total, values[:, start : start + LANES])
    return total


def square_sums(rows):
    wide = rows.astype(jnp.float32)
    return fold_lanes(wide * wide, jnp.add)


def to_scale(sums, width):
    return lax.rsqrt(sums / width + epsilon) / math.sqrt(width)


def kernel(dims, docs_hbm, eval_ref, ids_ref, row_out, bench_out, docs, held, labels, doc_scale,
           row_max, row_part, row_other, bench_acc, stage_col, stage_row, local_sem, send_sem, recv_sem):
    X, Z, Y = dims
    R, C = X * CORES, Z * Y
    row, col = lax.axis_index("row"), lax.axis_index("col")
    x, core = row // CORES, lax.rem(row, CORES)
    z, y = col // Y, lax.rem(col, Y)
    partner = x * CORES + (1 - core)
    n_docs, width = docs_hbm.shape
    piece = eval_ref.shape[0] // PARTS
    sizes = {"x": X, "y": Y, "z": Z}
    place = {"x": x, "y": y, "z": z}
    counter = [0]
    started = []

    def device(dim, step):
        moved = dict(place)
        moved[dim] = lax.rem(place[dim] + step + sizes[dim], sizes[dim])
        return {"row": moved["x"] * CORES + core, "col": moved["z"] * Y + moved["y"]}

    def send(src, dst, target):
        i = counter[0]
        counter[0] += 1
        copy = pltpu.make_async_remote_copy(
            src_ref=src, dst_ref=dst, send_sem=send_sem.at[i], recv_sem=recv_sem.at[i],
            device_id=target, device_id_type=MESH,
        )
        copy.start()
        started.append(copy)
        return copy

    barrier = pltpu.get_barrier_semaphore()
    for k in range(1, R):
        pl.semaphore_signal(barrier, inc=1, device_id={"row": lax.rem(row + k, R), "col": col}, device_id_type=MESH)
    for k in range(1, C):
        pl.semaphore_signal(barrier, inc=1, device_id={"row": row, "col": lax.rem(col + k, C)}, device_id_type=MESH)

    own_docs = pltpu.make_async_copy(docs_hbm, docs.at[core], local_sem.at[PARTS + 1])
    own_docs.start()
    locals_ = [
        pltpu.make_async_copy(eval_ref.at[pl.ds(q * piece, piece)], held.at[q, x, z, y], local_sem.at[q])
        for q in range(PARTS)
    ]
    locals_.append(pltpu.make_async_copy(ids_ref, labels.at[x, col], local_sem.at[PARTS]))
    for copy in locals_:
        copy.start()
    for copy in locals_:
        copy.wait()
    pl.semaphore_wait(barrier, R + C - 2)

    def gather(q, order):
        where = dict(place)
        for dim in order:
            n = sizes[dim]
            last = n // 2
            for step in range(1, last + 1):
                copies = []
                split = n % 2 == 0 and step == last and n > 2
                for sign in (1, -1):
                    if n == 2 and sign < 0:
                        continue
                    where[dim] = lax.rem(place[dim] - sign * (step - 1) + n, n)
                    ref = held.at[q, where["x"], where["z"], where["y"]]
                    if split:
                        half = width // 2
                        ref = held.at[q, where["x"], where["z"], where["y"], ..., pl.ds(0 if sign > 0 else half, half)]
                    copies.append(send(ref, ref, device(dim, sign)))
                yield
                for copy in copies:
                    copy.wait_recv()
            where[dim] = slice(None)

    runs = [gather(q, order) for q, order in enumerate(("xyz", "yxz", "zxy", "zyx"))]
    for run in runs:
        next(run, None)
    doc_copy = send(docs_hbm, docs.at[core], {"row": partner, "col": col})
    id_copies = [
        send(labels.at[x, col], labels.at[x, col], {"row": row, "col": lax.rem(col + k, C)}) for k in range(1, C)
    ]

    live = list(runs)
    first = True
    while live:
        keep = []
        for run in live:
            try:
                next(run)
                keep.append(run)
            except StopIteration:
                pass
        live = keep
        if first:
            first = False
            for copy in id_copies:
                copy.wait_recv()
            id_copies = [
                send(labels.at[x], labels.at[x], {"row": lax.rem(x + k, X) * CORES + core, "col": col})
                for k in range(1, X)
            ]
            own_docs.wait()
            doc_copy.wait_recv()
            for c in range(CORES):

                @pl.loop(0, n_docs // TILE)
                def _(t):
                    rows = pl.ds(pl.multiple_of(t * TILE, TILE), TILE)
                    sums = jnp.sum(square_sums(docs[c, rows, :]), axis=1, keepdims=True)
                    doc_scale[c, rows, :] = jnp.broadcast_to(to_scale(sums, width), (TILE, LANES))
                    row_max[c, rows, :] = jnp.full((TILE, LANES), -jnp.inf, jnp.float32)

            bench_acc[...] = jnp.full(bench_acc.shape, -jnp.inf, jnp.float32)
    for copy in id_copies:
        copy.wait_recv()

    owners = X * C
    chunk = owners * piece
    ids = labels[...].reshape(owners, ids_ref.shape[1]).astype(jnp.float32).astype(jnp.bfloat16)
    slot = lax.broadcasted_iota(jnp.int32, (ids_ref.shape[1], chunk), 0)
    lane = lax.broadcasted_iota(jnp.int32, (ids_ref.shape[1], chunk), 1)
    owner = lax.broadcasted_iota(jnp.int32, (owners, chunk), 0)
    owner_lane = lax.broadcasted_iota(jnp.int32, (owners, chunk), 1)
    bench = lax.broadcasted_iota(jnp.int32, (NBENCH, chunk), 0).astype(jnp.float32)
    for q in range(PARTS):
        questions = held[q].reshape(chunk, width)
        sums = jnp.sum(square_sums(questions).T, axis=0, keepdims=True)
        eval_scale = to_scale(sums, width)
        best = jnp.full((8, chunk), -jnp.inf, jnp.float32)
        for c in range(CORES):

            def absorb(t, best, c=c, questions=questions, eval_scale=eval_scale):
                rows = pl.ds(pl.multiple_of(t * TILE, TILE), TILE)
                products = lax.dot_general(
                    docs[c, rows, :], questions, (((1,), (1,)), ((), ())), preferred_element_type=jnp.float32
                )
                scored = products * eval_scale
                row_max[c, rows, :] = jnp.maximum(row_max[c, rows, :], fold_lanes(scored, jnp.maximum))
                scale = jnp.concatenate([doc_scale[c, rows, :]] * (chunk // LANES), axis=1)
                scored = scored * scale
                return jnp.maximum(best, jnp.max(scored.reshape(TILE // 8, 8, chunk), axis=0))

            best = lax.fori_loop(0, n_docs // TILE, absorb, best)
        column = jnp.max(best, axis=0, keepdims=True)
        spread = jnp.where(slot == q * piece + lax.rem(lane, piece), 1.0, 0.0).astype(jnp.bfloat16)
        placed = jnp.dot(ids, spread, preferred_element_type=jnp.float32)
        label = jnp.max(jnp.where(owner == owner_lane // piece, placed, -1.0), axis=0, keepdims=True)
        matched = jnp.where(bench == label, column, -jnp.inf)
        bench_acc[...] = jnp.maximum(bench_acc[...], fold_lanes(matched, jnp.maximum))

    mine = jnp.max(bench_acc[...].T, axis=0, keepdims=True)
    stage_col[col] = mine
    col_copies = [
        send(stage_col.at[col], stage_col.at[col], {"row": row, "col": lax.rem(col + k, C)}) for k in range(1, C)
    ]
    for c in range(CORES):
        for t in range(n_docs // LANES):
            rows = slice(t * LANES, (t + 1) * LANES)
            block = row_max[c, rows, :] * doc_scale[c, rows, :]
            row_part[c, t : t + 1, :] = jnp.max(block.T, axis=0, keepdims=True)
    row_copy = send(row_part.at[1 - core], row_other, {"row": partner, "col": col})
    for copy in col_copies:
        copy.wait_recv()
    mine = jnp.max(stage_col[...], axis=0)
    stage_row[row] = mine
    row_copies = [
        send(stage_row.at[row], stage_row.at[row], {"row": lax.rem(row + k, R), "col": col}) for k in range(1, R)
    ]
    row_copy.wait_recv()
    row_out[...] = jnp.maximum(row_part[core], row_other[...])
    for copy in row_copies:
        copy.wait_recv()
    bench_out[...] = jnp.max(stage_row[...], axis=0)
    for copy in started:
        copy.wait_send()


def split_col(size):
    best = 1
    for candidate in range(1, size + 1):
        if size % candidate == 0 and candidate * candidate <= size:
            best = candidate
    return best


def body(dims, train_docs, eval_rows, bench_ids):
    X, Z, Y = dims
    n_docs, width = train_docs.shape
    own = eval_rows.shape[0]
    R, C = X * CORES, Z * Y
    owners = X * C
    copies = 4 * PARTS * (X + Y + Z) + 2 * (R + C) + 4
    f32 = jnp.float32
    row_best, bench_best = pl.pallas_call(
        functools.partial(kernel, dims),
        out_shape=(
            jax.ShapeDtypeStruct((n_docs // LANES, LANES), f32),
            jax.ShapeDtypeStruct((1, NBENCH), f32),
        ),
        in_specs=[
            pl.BlockSpec(memory_space=pl.ANY),
            pl.BlockSpec(memory_space=pltpu.VMEM),
            pl.BlockSpec(memory_space=pltpu.VMEM),
        ],
        out_specs=(pl.BlockSpec(memory_space=pltpu.VMEM), pl.BlockSpec(memory_space=pltpu.VMEM)),
        scratch_shapes=[
            pltpu.VMEM((CORES, n_docs, width), train_docs.dtype),
            pltpu.VMEM((PARTS, X, Z, Y, own // PARTS, width), eval_rows.dtype),
            pltpu.VMEM((X, C, 1, own), jnp.int32),
            pltpu.VMEM((CORES, n_docs, LANES), f32),
            pltpu.VMEM((CORES, n_docs, LANES), f32),
            pltpu.VMEM((CORES, n_docs // LANES, LANES), f32),
            pltpu.VMEM((n_docs // LANES, LANES), f32),
            pltpu.VMEM((NBENCH, LANES), f32),
            pltpu.VMEM((C, 1, NBENCH), f32),
            pltpu.VMEM((R, 1, NBENCH), f32),
            pltpu.SemaphoreType.DMA((PARTS + 2,)),
            pltpu.SemaphoreType.DMA((copies,)),
            pltpu.SemaphoreType.DMA((copies,)),
        ],
        compiler_params=pltpu.CompilerParams(
            collective_id=0, has_side_effects=True, vmem_limit_bytes=48 * 1024 * 1024
        ),
    )(train_docs, eval_rows, bench_ids.reshape(1, own))
    return row_best.reshape(n_docs), bench_best.reshape(NBENCH)


def solution(mesh):
    columns = mesh.shape["col"]
    Y = split_col(columns)
    dims = (mesh.shape["row"] // CORES, columns // Y, Y)
    in_specs = (P(("row", "col"), None), P(("row", "col"), None), P(("row", "col"), None))
    out_specs = (P(("row", "col")), P())
    return jax.shard_map(
        functools.partial(body, dims), mesh=mesh, in_specs=in_specs, out_specs=out_specs, check_vma=False
    )
```

```python
import functools
import math

import jax
import jax.numpy as jnp
from jax import lax
from jax.experimental import pallas as pl
from jax.experimental.pallas import tpu as pltpu
from jax.sharding import PartitionSpec as P

NBENCH = 128
CORES = 2
PARTS = 4
TILE = 256
ROWS = 1024
LANES = 128

epsilon = 1e-06
MESH = pl.DeviceIdType.MESH


def fold_lanes(values, op):
    total = values[:, :LANES]
    for start in range(LANES, values.shape[1], LANES):
        total = op(total, values[:, start : start + LANES])
    return total


def square_sums(rows):
    wide = rows.astype(jnp.float32)
    return fold_lanes(wide * wide, jnp.add)


def to_scale(sums, width):
    return lax.rsqrt(sums / width + epsilon) / math.sqrt(width)


def kernel(dims, docs_hbm, eval_ref, ids_ref, row_out, bench_out, docs, held, labels, doc_scale,
           row_max, row_part, row_other, bench_acc, stage_col, stage_row, local_sem, send_sem, recv_sem):
    X, Z, Y = dims
    R, C = X * CORES, Z * Y
    row, col = lax.axis_index("row"), lax.axis_index("col")
    x, core = row // CORES, lax.rem(row, CORES)
    z, y = col // Y, lax.rem(col, Y)
    partner = x * CORES + (1 - core)
    n_docs, width = docs_hbm.shape
    piece = eval_ref.shape[0] // PARTS
    sizes = {"x": X, "y": Y, "z": Z}
    place = {"x": x, "y": y, "z": z}
    counter = [0]
    started = []

    def device(dim, step):
        moved = dict(place)
        moved[dim] = lax.rem(place[dim] + step + sizes[dim], sizes[dim])
        return {"row": moved["x"] * CORES + core, "col": moved["z"] * Y + moved["y"]}

    def send(src, dst, target):
        i = counter[0]
        counter[0] += 1
        copy = pltpu.make_async_remote_copy(
            src_ref=src, dst_ref=dst, send_sem=send_sem.at[i], recv_sem=recv_sem.at[i],
            device_id=target, device_id_type=MESH,
        )
        copy.start()
        started.append(copy)
        return copy

    barrier = pltpu.get_barrier_semaphore()
    for k in range(1, R):
        pl.semaphore_signal(barrier, inc=1, device_id={"row": lax.rem(row + k, R), "col": col}, device_id_type=MESH)
    for k in range(1, C):
        pl.semaphore_signal(barrier, inc=1, device_id={"row": row, "col": lax.rem(col + k, C)}, device_id_type=MESH)

    own_docs = pltpu.make_async_copy(docs_hbm, docs.at[core], local_sem.at[PARTS + 1])
    own_docs.start()
    locals_ = [
        pltpu.make_async_copy(eval_ref.at[pl.ds(q * piece, piece)], held.at[q, x, z, y], local_sem.at[q])
        for q in range(PARTS)
    ]
    locals_.append(pltpu.make_async_copy(ids_ref, labels.at[x, col], local_sem.at[PARTS]))
    for copy in locals_:
        copy.start()
    for copy in locals_:
        copy.wait()
    pl.semaphore_wait(barrier, R + C - 2)

    def gather(q, order):
        where = dict(place)
        for dim in order:
            n = sizes[dim]
            last = n // 2
            for step in range(1, last + 1):
                copies = []
                split = n % 2 == 0 and step == last and n > 2
                for sign in (1, -1):
                    if n == 2 and sign < 0:
                        continue
                    where[dim] = lax.rem(place[dim] - sign * (step - 1) + n, n)
                    ref = held.at[q, where["x"], where["z"], where["y"]]
                    if split:
                        half = width // 2
                        ref = held.at[q, where["x"], where["z"], where["y"], ..., pl.ds(0 if sign > 0 else half, half)]
                    copies.append(send(ref, ref, device(dim, sign)))
                yield
                for copy in copies:
                    copy.wait_recv()
            where[dim] = slice(None)

    orders = ("zxy", "zyx", "xyz", "yxz")
    runs = [gather(q, order) for q, order in enumerate(orders)]
    for run in runs:
        next(run, None)
    doc_copy = send(docs_hbm, docs.at[core], {"row": partner, "col": col})
    id_copies = [
        send(labels.at[x, col], labels.at[x, col], {"row": row, "col": lax.rem(col + k, C)}) for k in range(1, C)
    ]

    live = list(runs)
    first, turn = True, 0
    while live:
        keep = []
        for run in live:
            try:
                next(run)
                keep.append(run)
            except StopIteration:
                pass
        live = keep
        turn += 1
        if turn == 2:
            for copy in id_copies:
                copy.wait_recv()
            id_copies = [
                send(labels.at[x], labels.at[x], {"row": lax.rem(x + k, X) * CORES + core, "col": col})
                for k in range(1, X)
            ]
        if first:
            first = False
            own_docs.wait()
            doc_copy.wait_recv()
            for c in range(CORES):

                @pl.loop(0, n_docs // TILE)
                def _(t):
                    rows = pl.ds(pl.multiple_of(t * TILE, TILE), TILE)
                    sums = jnp.sum(square_sums(docs[c, rows, :]), axis=1, keepdims=True)
                    doc_scale[c, rows, :] = jnp.broadcast_to(to_scale(sums, width), (TILE, LANES))
                    row_max[c, rows, :] = jnp.full((TILE, LANES), -jnp.inf, jnp.float32)

            bench_acc[...] = jnp.full(bench_acc.shape, -jnp.inf, jnp.float32)
    for copy in id_copies:
        copy.wait_recv()

    tall = math.gcd(n_docs, ROWS)
    owners = X * C
    chunk = owners * piece
    ids = labels[...].reshape(owners, ids_ref.shape[1]).astype(jnp.float32).astype(jnp.bfloat16)
    slot = lax.broadcasted_iota(jnp.int32, (ids_ref.shape[1], chunk), 0)
    lane = lax.broadcasted_iota(jnp.int32, (ids_ref.shape[1], chunk), 1)
    owner = lax.broadcasted_iota(jnp.int32, (owners, chunk), 0)
    owner_lane = lax.broadcasted_iota(jnp.int32, (owners, chunk), 1)
    bench = lax.broadcasted_iota(jnp.int32, (NBENCH, chunk), 0).astype(jnp.float32)
    for q in range(PARTS):
        questions = held[q].reshape(chunk, width)
        sums = jnp.sum(square_sums(questions).T, axis=0, keepdims=True)
        eval_scale = to_scale(sums, width)
        best = jnp.full((8, chunk), -jnp.inf, jnp.float32)
        for c in range(CORES):

            def absorb(t, best, c=c, questions=questions, eval_scale=eval_scale):
                rows = pl.ds(pl.multiple_of(t * tall, tall), tall)
                products = lax.dot_general(
                    docs[c, rows, :], questions, (((1,), (1,)), ((), ())), preferred_element_type=jnp.float32
                )
                scored = products * eval_scale
                row_max[c, rows, :] = jnp.maximum(row_max[c, rows, :], fold_lanes(scored, jnp.maximum))
                scale = jnp.concatenate([doc_scale[c, rows, :]] * (chunk // LANES), axis=1)
                scored = scored * scale
                return jnp.maximum(best, jnp.max(scored.reshape(tall // 8, 8, chunk), axis=0))

            best = lax.fori_loop(0, n_docs // tall, absorb, best)
        column = jnp.max(best, axis=0, keepdims=True)
        spread = jnp.where(slot == q * piece + lax.rem(lane, piece), 1.0, 0.0).astype(jnp.bfloat16)
        placed = jnp.dot(ids, spread, preferred_element_type=jnp.float32)
        label = jnp.max(jnp.where(owner == owner_lane // piece, placed, -1.0), axis=0, keepdims=True)
        matched = jnp.where(bench == label, column, -jnp.inf)
        bench_acc[...] = jnp.maximum(bench_acc[...], fold_lanes(matched, jnp.maximum))

    mine = jnp.max(bench_acc[...].T, axis=0, keepdims=True)
    stage_col[col] = mine
    col_copies = [
        send(stage_col.at[col], stage_col.at[col], {"row": row, "col": lax.rem(col + k, C)}) for k in range(1, C)
    ]
    for c in range(CORES):
        for t in range(n_docs // LANES):
            rows = slice(t * LANES, (t + 1) * LANES)
            block = row_max[c, rows, :] * doc_scale[c, rows, :]
            row_part[c, t : t + 1, :] = jnp.max(block.T, axis=0, keepdims=True)
    row_copy = send(row_part.at[1 - core], row_other, {"row": partner, "col": col})
    for copy in col_copies:
        copy.wait_recv()
    mine = jnp.max(stage_col[...], axis=0)
    stage_row[row] = mine
    row_copies = [
        send(stage_row.at[row], stage_row.at[row], {"row": lax.rem(row + k, R), "col": col}) for k in range(1, R)
    ]
    row_copy.wait_recv()
    row_out[...] = jnp.maximum(row_part[core], row_other[...])
    for copy in row_copies:
        copy.wait_recv()
    bench_out[...] = jnp.max(stage_row[...], axis=0)
    for copy in started:
        copy.wait_send()


def split_col(size):
    best = 1
    for candidate in range(1, size + 1):
        if size % candidate == 0 and candidate * candidate <= size:
            best = candidate
    return best


def body(dims, train_docs, eval_rows, bench_ids):
    X, Z, Y = dims
    n_docs, width = train_docs.shape
    own = eval_rows.shape[0]
    R, C = X * CORES, Z * Y
    owners = X * C
    copies = 4 * PARTS * (X + Y + Z) + 2 * (R + C) + 4
    f32 = jnp.float32
    row_best, bench_best = pl.pallas_call(
        functools.partial(kernel, dims),
        out_shape=(
            jax.ShapeDtypeStruct((n_docs // LANES, LANES), f32),
            jax.ShapeDtypeStruct((1, NBENCH), f32),
        ),
        in_specs=[
            pl.BlockSpec(memory_space=pltpu.HBM),
            pl.BlockSpec(memory_space=pltpu.HBM),
            pl.BlockSpec(memory_space=pltpu.HBM),
        ],
        out_specs=(pl.BlockSpec(memory_space=pltpu.VMEM), pl.BlockSpec(memory_space=pltpu.VMEM)),
        scratch_shapes=[
            pltpu.VMEM((CORES, n_docs, width), train_docs.dtype),
            pltpu.VMEM((PARTS, X, Z, Y, own // PARTS, width), eval_rows.dtype),
            pltpu.VMEM((X, C, 1, own), jnp.int32),
            pltpu.VMEM((CORES, n_docs, LANES), f32),
            pltpu.VMEM((CORES, n_docs, LANES), f32),
            pltpu.VMEM((CORES, n_docs // LANES, LANES), f32),
            pltpu.VMEM((n_docs // LANES, LANES), f32),
            pltpu.VMEM((NBENCH, LANES), f32),
            pltpu.VMEM((C, 1, NBENCH), f32),
            pltpu.VMEM((R, 1, NBENCH), f32),
            pltpu.SemaphoreType.DMA((PARTS + 2,)),
            pltpu.SemaphoreType.DMA((copies,)),
            pltpu.SemaphoreType.DMA((copies,)),
        ],
        compiler_params=pltpu.CompilerParams(
            collective_id=0, has_side_effects=True, vmem_limit_bytes=48 * 1024 * 1024
        ),
    )(train_docs, eval_rows, bench_ids.reshape(1, own))
    return row_best.reshape(n_docs), bench_best.reshape(NBENCH)


def solution(mesh):
    columns = mesh.shape["col"]
    Y = split_col(columns)
    dims = (mesh.shape["row"] // CORES, columns // Y, Y)
    in_specs = (P(("row", "col"), None), P(("row", "col"), None), P(("row", "col"), None))
    out_specs = (P(("row", "col")), P())
    return jax.shard_map(
        functools.partial(body, dims), mesh=mesh, in_specs=in_specs, out_specs=out_specs, check_vma=False
    )
```

```python
import functools
import math

import jax
import jax.numpy as jnp
from jax import lax
from jax.experimental import pallas as pl
from jax.experimental.pallas import tpu as pltpu
from jax.sharding import PartitionSpec as P

NBENCH = 128
CORES = 2
PARTS = 4
TILE = 256
ROWS = 1024
ORDERS = ("zxy", "zyx", "xyz", "yxz")
LANES = 128

epsilon = 1e-06
MESH = pl.DeviceIdType.MESH


def fold_lanes(values, op):
    total = values[:, :LANES]
    for start in range(LANES, values.shape[1], LANES):
        total = op(total, values[:, start : start + LANES])
    return total


def square_sums(rows):
    wide = rows.astype(jnp.float32)
    return fold_lanes(wide * wide, jnp.add)


def to_scale(sums, width):
    return lax.rsqrt(sums / width + epsilon) / math.sqrt(width)


def kernel(dims, docs_hbm, eval_ref, ids_ref, row_out, bench_out, docs, held, labels, doc_scale,
           row_max, row_part, row_other, bench_acc, stage_col, stage_row, local_sem, send_sem, recv_sem):
    X, Z, Y = dims
    R, C = X * CORES, Z * Y
    row, col = lax.axis_index("row"), lax.axis_index("col")
    x, core = row // CORES, lax.rem(row, CORES)
    z, y = col // Y, lax.rem(col, Y)
    partner = x * CORES + (1 - core)
    n_docs, width = docs_hbm.shape
    piece = eval_ref.shape[0] // PARTS
    sizes = {"x": X, "y": Y, "z": Z}
    place = {"x": x, "y": y, "z": z}
    counter = [0]
    started = []

    def device(dim, step):
        moved = dict(place)
        moved[dim] = lax.rem(place[dim] + step + sizes[dim], sizes[dim])
        return {"row": moved["x"] * CORES + core, "col": moved["z"] * Y + moved["y"]}

    def send(src, dst, target):
        i = counter[0]
        counter[0] += 1
        copy = pltpu.make_async_remote_copy(
            src_ref=src, dst_ref=dst, send_sem=send_sem.at[i], recv_sem=recv_sem.at[i],
            device_id=target, device_id_type=MESH,
        )
        copy.start()
        started.append(copy)
        return copy

    barrier = pltpu.get_barrier_semaphore()
    for k in range(1, R):
        pl.semaphore_signal(barrier, inc=1, device_id={"row": lax.rem(row + k, R), "col": col}, device_id_type=MESH)
    for k in range(1, C):
        pl.semaphore_signal(barrier, inc=1, device_id={"row": row, "col": lax.rem(col + k, C)}, device_id_type=MESH)

    own_docs = pltpu.make_async_copy(docs_hbm, docs.at[core], local_sem.at[PARTS + 1])
    own_docs.start()
    locals_ = [
        pltpu.make_async_copy(eval_ref.at[pl.ds(q * piece, piece)], held.at[q, x, z, y], local_sem.at[q])
        for q in range(PARTS)
    ]
    locals_.append(pltpu.make_async_copy(ids_ref, labels.at[x, col], local_sem.at[PARTS]))
    for copy in locals_:
        copy.start()
    for copy in locals_:
        copy.wait()
    pl.semaphore_wait(barrier, R + C - 2)

    waiting = []

    def emit(q, fixed, dim, later, step):
        n = sizes[dim]
        last = n // 2
        if step > last:
            return
        split = n % 2 == 0 and step == last and n > 2
        copies, arrivals = [], []
        for sign in (1, -1) if n > 2 else (1,):
            where = {**place, **fixed, dim: lax.rem(place[dim] - sign * (step - 1) + n, n)}
            at = (q, where["x"], where["z"], where["y"])
            if split:
                half = width // 2
                at += (slice(None), pl.ds(0 if sign > 0 else half, half))
            copies.append(send(held.at[at], held.at[at], device(dim, sign)))
            arrivals.append(lax.rem(place[dim] - sign * step + n, n))
        waiting.append((q, fixed, dim, later, step, copies, arrivals[:1] if split else arrivals))

    def advance():
        q, fixed, dim, later, step, copies, arrivals = waiting.pop(0)
        for copy in copies:
            copy.wait_recv()
        emit(q, fixed, dim, later, step + 1)
        for position in arrivals:
            for k, follow in enumerate(later):
                emit(q, {**fixed, dim: position}, follow, later[k + 1 :], 1)

    for level in range(3):
        for q, order in enumerate(ORDERS):
            emit(q, {}, order[level], order[level + 1 :], 1)
        if level == 0:
            doc_copy = send(docs_hbm, docs.at[core], {"row": partner, "col": col})
            id_copies = [
                send(labels.at[x, col], labels.at[x, col], {"row": row, "col": lax.rem(col + k, C)})
                for k in range(1, C)
            ]

    for _ in range(len(waiting)):
        advance()
    for copy in id_copies:
        copy.wait_recv()
    id_copies = [
        send(labels.at[x], labels.at[x], {"row": lax.rem(x + k, X) * CORES + core, "col": col}) for k in range(1, X)
    ]
    own_docs.wait()
    doc_copy.wait_recv()
    bench_acc[...] = jnp.full(bench_acc.shape, -jnp.inf, jnp.float32)
    for c in range(CORES):

        @pl.loop(0, n_docs // TILE)
        def _(t):
            rows = pl.ds(pl.multiple_of(t * TILE, TILE), TILE)
            sums = jnp.sum(square_sums(docs[c, rows, :]), axis=1, keepdims=True)
            doc_scale[c, rows, :] = jnp.broadcast_to(to_scale(sums, width), (TILE, LANES))
            row_max[c, rows, :] = jnp.full((TILE, LANES), -jnp.inf, jnp.float32)

        for _ in range(len(waiting) // 2):
            advance()
    while waiting:
        advance()
    for copy in id_copies:
        copy.wait_recv()

    tall = math.gcd(n_docs, ROWS)
    owners = X * C
    chunk = owners * piece
    ids = labels[...].reshape(owners, ids_ref.shape[1]).astype(jnp.float32).astype(jnp.bfloat16)
    slot = lax.broadcasted_iota(jnp.int32, (ids_ref.shape[1], chunk), 0)
    lane = lax.broadcasted_iota(jnp.int32, (ids_ref.shape[1], chunk), 1)
    owner = lax.broadcasted_iota(jnp.int32, (owners, chunk), 0)
    owner_lane = lax.broadcasted_iota(jnp.int32, (owners, chunk), 1)
    bench = lax.broadcasted_iota(jnp.int32, (NBENCH, chunk), 0).astype(jnp.float32)
    for q in range(PARTS):
        questions = held[q].reshape(chunk, width)
        sums = jnp.sum(square_sums(questions).T, axis=0, keepdims=True)
        eval_scale = to_scale(sums, width)
        best = jnp.full((8, chunk), -jnp.inf, jnp.float32)
        for c in range(CORES):

            def absorb(t, best, c=c, questions=questions, eval_scale=eval_scale):
                rows = pl.ds(pl.multiple_of(t * tall, tall), tall)
                products = lax.dot_general(
                    docs[c, rows, :], questions, (((1,), (1,)), ((), ())), preferred_element_type=jnp.float32
                )
                scored = products * eval_scale
                row_max[c, rows, :] = jnp.maximum(row_max[c, rows, :], fold_lanes(scored, jnp.maximum))
                scale = jnp.concatenate([doc_scale[c, rows, :]] * (chunk // LANES), axis=1)
                scored = scored * scale
                return jnp.maximum(best, jnp.max(scored.reshape(tall // 8, 8, chunk), axis=0))

            best = lax.fori_loop(0, n_docs // tall, absorb, best)
        column = jnp.max(best, axis=0, keepdims=True)
        spread = jnp.where(slot == q * piece + lax.rem(lane, piece), 1.0, 0.0).astype(jnp.bfloat16)
        placed = jnp.dot(ids, spread, preferred_element_type=jnp.float32)
        label = jnp.max(jnp.where(owner == owner_lane // piece, placed, -1.0), axis=0, keepdims=True)
        matched = jnp.where(bench == label, column, -jnp.inf)
        bench_acc[...] = jnp.maximum(bench_acc[...], fold_lanes(matched, jnp.maximum))

    mine = jnp.max(bench_acc[...].T, axis=0, keepdims=True)
    stage_col[col] = mine
    col_copies = [
        send(stage_col.at[col], stage_col.at[col], {"row": row, "col": lax.rem(col + k, C)}) for k in range(1, C)
    ]
    for c in range(CORES):
        for t in range(n_docs // LANES):
            rows = slice(t * LANES, (t + 1) * LANES)
            block = row_max[c, rows, :] * doc_scale[c, rows, :]
            row_part[c, t : t + 1, :] = jnp.max(block.T, axis=0, keepdims=True)
    row_copy = send(row_part.at[1 - core], row_other, {"row": partner, "col": col})
    for copy in col_copies:
        copy.wait_recv()
    mine = jnp.max(stage_col[...], axis=0)
    stage_row[row] = mine
    row_copies = [
        send(stage_row.at[row], stage_row.at[row], {"row": lax.rem(row + k, R), "col": col}) for k in range(1, R)
    ]
    row_copy.wait_recv()
    row_out[...] = jnp.maximum(row_part[core], row_other[...])
    for copy in row_copies:
        copy.wait_recv()
    bench_out[...] = jnp.max(stage_row[...], axis=0)
    for copy in started:
        copy.wait_send()


def split_col(size):
    best = 1
    for candidate in range(1, size + 1):
        if size % candidate == 0 and candidate * candidate <= size:
            best = candidate
    return best


def body(dims, train_docs, eval_rows, bench_ids):
    X, Z, Y = dims
    n_docs, width = train_docs.shape
    own = eval_rows.shape[0]
    R, C = X * CORES, Z * Y
    owners = X * C
    sizes = {"x": X, "y": Y, "z": Z}
    copies = 2 * (R + C) + 4
    for a, b, c in ORDERS:
        copies += sizes[a] * (1 + sizes[b] * (1 + sizes[c]))
    f32 = jnp.float32
    row_best, bench_best = pl.pallas_call(
        functools.partial(kernel, dims),
        out_shape=(
            jax.ShapeDtypeStruct((n_docs // LANES, LANES), f32),
            jax.ShapeDtypeStruct((1, NBENCH), f32),
        ),
        in_specs=[
            pl.BlockSpec(memory_space=pltpu.HBM),
            pl.BlockSpec(memory_space=pltpu.HBM),
            pl.BlockSpec(memory_space=pltpu.HBM),
        ],
        out_specs=(pl.BlockSpec(memory_space=pltpu.VMEM), pl.BlockSpec(memory_space=pltpu.VMEM)),
        scratch_shapes=[
            pltpu.VMEM((CORES, n_docs, width), train_docs.dtype),
            pltpu.VMEM((PARTS, X, Z, Y, own // PARTS, width), eval_rows.dtype),
            pltpu.VMEM((X, C, 1, own), jnp.int32),
            pltpu.VMEM((CORES, n_docs, LANES), f32),
            pltpu.VMEM((CORES, n_docs, LANES), f32),
            pltpu.VMEM((CORES, n_docs // LANES, LANES), f32),
            pltpu.VMEM((n_docs // LANES, LANES), f32),
            pltpu.VMEM((NBENCH, LANES), f32),
            pltpu.VMEM((C, 1, NBENCH), f32),
            pltpu.VMEM((R, 1, NBENCH), f32),
            pltpu.SemaphoreType.DMA((PARTS + 2,)),
            pltpu.SemaphoreType.DMA((copies,)),
            pltpu.SemaphoreType.DMA((copies,)),
        ],
        compiler_params=pltpu.CompilerParams(
            collective_id=0, has_side_effects=True, vmem_limit_bytes=48 * 1024 * 1024
        ),
    )(train_docs, eval_rows, bench_ids.reshape(1, own))
    return row_best.reshape(n_docs), bench_best.reshape(NBENCH)


def solution(mesh):
    columns = mesh.shape["col"]
    Y = split_col(columns)
    dims = (mesh.shape["row"] // CORES, columns // Y, Y)
    in_specs = (P(("row", "col"), None), P(("row", "col"), None), P(("row", "col"), None))
    out_specs = (P(("row", "col")), P())
    return jax.shard_map(
        functools.partial(body, dims), mesh=mesh, in_specs=in_specs, out_specs=out_specs, check_vma=False
    )
```

```python
import functools
import math

import jax
import jax.numpy as jnp
from jax import lax
from jax.experimental import pallas as pl
from jax.experimental.pallas import tpu as pltpu
from jax.sharding import PartitionSpec as P

NBENCH = 128
CORES = 2
PARTS = 4
TILE = 256
ROWS = 1024
ORDERS = ("zxy", "zyx", "xyz", "yxz")
LANES = 128

epsilon = 1e-06
MESH = pl.DeviceIdType.MESH


def fold_lanes(values, op):
    total = values[:, :LANES]
    for start in range(LANES, values.shape[1], LANES):
        total = op(total, values[:, start : start + LANES])
    return total


def square_sums(rows):
    wide = rows.astype(jnp.float32)
    return fold_lanes(wide * wide, jnp.add)


def to_scale(sums, width):
    return lax.rsqrt(sums / width + epsilon) / math.sqrt(width)


def kernel(dims, docs_hbm, eval_ref, ids_ref, row_out, bench_out, docs, held, labels, doc_scale,
           row_max, row_part, row_other, bench_acc, stage_col, stage_row, local_sem, send_sem, recv_sem):
    X, Z, Y = dims
    R, C = X * CORES, Z * Y
    row, col = lax.axis_index("row"), lax.axis_index("col")
    x, core = row // CORES, lax.rem(row, CORES)
    z, y = col // Y, lax.rem(col, Y)
    partner = x * CORES + (1 - core)
    n_docs, width = docs_hbm.shape
    piece = eval_ref.shape[0] // PARTS
    sizes = {"x": X, "y": Y, "z": Z}
    place = {"x": x, "y": y, "z": z}
    counter = [0]
    started = []

    def device(dim, step):
        moved = dict(place)
        moved[dim] = lax.rem(place[dim] + step + sizes[dim], sizes[dim])
        return {"row": moved["x"] * CORES + core, "col": moved["z"] * Y + moved["y"]}

    def send(src, dst, target):
        i = counter[0]
        counter[0] += 1
        copy = pltpu.make_async_remote_copy(
            src_ref=src, dst_ref=dst, send_sem=send_sem.at[i], recv_sem=recv_sem.at[i],
            device_id=target, device_id_type=MESH,
        )
        copy.start()
        started.append(copy)
        return copy

    barrier = pltpu.get_barrier_semaphore()
    for k in range(1, R):
        pl.semaphore_signal(barrier, inc=1, device_id={"row": lax.rem(row + k, R), "col": col}, device_id_type=MESH)
    for k in range(1, C):
        pl.semaphore_signal(barrier, inc=1, device_id={"row": row, "col": lax.rem(col + k, C)}, device_id_type=MESH)

    own_docs = pltpu.make_async_copy(docs_hbm, docs.at[core], local_sem.at[PARTS + 1])
    own_docs.start()
    locals_ = [
        pltpu.make_async_copy(eval_ref.at[pl.ds(q * piece, piece)], held.at[q, x, z, y], local_sem.at[q])
        for q in range(PARTS)
    ]
    locals_.append(pltpu.make_async_copy(ids_ref, labels.at[x, col], local_sem.at[PARTS]))
    for copy in locals_:
        copy.start()
    for copy in locals_:
        copy.wait()
    pl.semaphore_wait(barrier, R + C - 2)

    waiting = []

    def emit(q, fixed, dim, later, step):
        n = sizes[dim]
        last = n // 2
        if step > last:
            return
        split = n % 2 == 0 and step == last and n > 2
        copies, arrivals = [], []
        for sign in (1, -1) if n > 2 else (1,):
            where = {**place, **fixed, dim: lax.rem(place[dim] - sign * (step - 1) + n, n)}
            at = (q, where["x"], where["z"], where["y"])
            if split:
                half = width // 2
                at += (slice(None), pl.ds(0 if sign > 0 else half, half))
            copies.append(send(held.at[at], held.at[at], device(dim, sign)))
            arrivals.append(lax.rem(place[dim] - sign * step + n, n))
        waiting.append((q, fixed, dim, later, step, copies, arrivals[:1] if split else arrivals))

    def forwarding():
        return [event for event in waiting if event[3] or event[4] < sizes[event[2]] // 2]

    def advance():
        event = forwarding()[0]
        waiting[:] = [other for other in waiting if other is not event]
        q, fixed, dim, later, step, copies, arrivals = event
        for copy in copies:
            copy.wait_recv()
        emit(q, fixed, dim, later, step + 1)
        for position in arrivals:
            for k, follow in enumerate(later):
                emit(q, {**fixed, dim: position}, follow, later[k + 1 :], 1)

    for level in range(3):
        for q, order in enumerate(ORDERS):
            emit(q, {}, order[level], order[level + 1 :], 1)
        if level == 0:
            doc_copy = send(docs_hbm, docs.at[core], {"row": partner, "col": col})
            id_copies = [
                send(labels.at[x, col], labels.at[x, col], {"row": row, "col": lax.rem(col + k, C)})
                for k in range(1, C)
            ]

    for _ in range(len(forwarding())):
        advance()
    for copy in id_copies:
        copy.wait_recv()
    id_copies = [
        send(labels.at[x], labels.at[x], {"row": lax.rem(x + k, X) * CORES + core, "col": col}) for k in range(1, X)
    ]
    own_docs.wait()
    doc_copy.wait_recv()
    bench_acc[...] = jnp.full(bench_acc.shape, -jnp.inf, jnp.float32)
    for c in range(CORES):

        @pl.loop(0, n_docs // TILE)
        def _(t):
            rows = pl.ds(pl.multiple_of(t * TILE, TILE), TILE)
            sums = jnp.sum(square_sums(docs[c, rows, :]), axis=1, keepdims=True)
            doc_scale[c, rows, :] = jnp.broadcast_to(to_scale(sums, width), (TILE, LANES))
            row_max[c, rows, :] = jnp.full((TILE, LANES), -jnp.inf, jnp.float32)

        for _ in range(len(forwarding()) // 2):
            advance()
    while forwarding():
        advance()
    for copy in id_copies:
        copy.wait_recv()

    tall = math.gcd(n_docs, ROWS)
    owners = X * C
    chunk = owners * piece
    ids = labels[...].reshape(owners, ids_ref.shape[1]).astype(jnp.float32).astype(jnp.bfloat16)
    slot = lax.broadcasted_iota(jnp.int32, (ids_ref.shape[1], chunk), 0)
    lane = lax.broadcasted_iota(jnp.int32, (ids_ref.shape[1], chunk), 1)
    owner = lax.broadcasted_iota(jnp.int32, (owners, chunk), 0)
    owner_lane = lax.broadcasted_iota(jnp.int32, (owners, chunk), 1)
    bench = lax.broadcasted_iota(jnp.int32, (NBENCH, chunk), 0).astype(jnp.float32)
    for q in range(PARTS):
        for event in waiting:
            if event[0] == q:
                for copy in event[5]:
                    copy.wait_recv()
        questions = held[q].reshape(chunk, width)
        sums = jnp.sum(square_sums(questions).T, axis=0, keepdims=True)
        eval_scale = to_scale(sums, width)
        best = jnp.full((8, chunk), -jnp.inf, jnp.float32)
        for c in range(CORES):

            def absorb(t, best, c=c, questions=questions, eval_scale=eval_scale):
                rows = pl.ds(pl.multiple_of(t * tall, tall), tall)
                products = lax.dot_general(
                    docs[c, rows, :], questions, (((1,), (1,)), ((), ())), preferred_element_type=jnp.float32
                )
                scored = products * eval_scale
                row_max[c, rows, :] = jnp.maximum(row_max[c, rows, :], fold_lanes(scored, jnp.maximum))
                scale = jnp.concatenate([doc_scale[c, rows, :]] * (chunk // LANES), axis=1)
                scored = scored * scale
                return jnp.maximum(best, jnp.max(scored.reshape(tall // 8, 8, chunk), axis=0))

            best = lax.fori_loop(0, n_docs // tall, absorb, best)
        column = jnp.max(best, axis=0, keepdims=True)
        spread = jnp.where(slot == q * piece + lax.rem(lane, piece), 1.0, 0.0).astype(jnp.bfloat16)
        placed = jnp.dot(ids, spread, preferred_element_type=jnp.float32)
        label = jnp.max(jnp.where(owner == owner_lane // piece, placed, -1.0), axis=0, keepdims=True)
        matched = jnp.where(bench == label, column, -jnp.inf)
        bench_acc[...] = jnp.maximum(bench_acc[...], fold_lanes(matched, jnp.maximum))

    mine = jnp.max(bench_acc[...].T, axis=0, keepdims=True)
    stage_col[col] = mine
    col_copies = [
        send(stage_col.at[col], stage_col.at[col], {"row": row, "col": lax.rem(col + k, C)}) for k in range(1, C)
    ]
    for c in range(CORES):
        for t in range(n_docs // LANES):
            rows = slice(t * LANES, (t + 1) * LANES)
            block = row_max[c, rows, :] * doc_scale[c, rows, :]
            row_part[c, t : t + 1, :] = jnp.max(block.T, axis=0, keepdims=True)
    row_copy = send(row_part.at[1 - core], row_other, {"row": partner, "col": col})
    for copy in col_copies:
        copy.wait_recv()
    mine = jnp.max(stage_col[...], axis=0)
    stage_row[row] = mine
    row_copies = [
        send(stage_row.at[row], stage_row.at[row], {"row": lax.rem(row + k, R), "col": col}) for k in range(1, R)
    ]
    row_copy.wait_recv()
    row_out[...] = jnp.maximum(row_part[core], row_other[...])
    for copy in row_copies:
        copy.wait_recv()
    bench_out[...] = jnp.max(stage_row[...], axis=0)
    for copy in started:
        copy.wait_send()


def split_col(size):
    best = 1
    for candidate in range(1, size + 1):
        if size % candidate == 0 and candidate * candidate <= size:
            best = candidate
    return best


def body(dims, train_docs, eval_rows, bench_ids):
    X, Z, Y = dims
    n_docs, width = train_docs.shape
    own = eval_rows.shape[0]
    R, C = X * CORES, Z * Y
    owners = X * C
    sizes = {"x": X, "y": Y, "z": Z}
    copies = 2 * (R + C) + 4
    for a, b, c in ORDERS:
        copies += sizes[a] * (1 + sizes[b] * (1 + sizes[c]))
    f32 = jnp.float32
    row_best, bench_best = pl.pallas_call(
        functools.partial(kernel, dims),
        out_shape=(
            jax.ShapeDtypeStruct((n_docs // LANES, LANES), f32),
            jax.ShapeDtypeStruct((1, NBENCH), f32),
        ),
        in_specs=[
            pl.BlockSpec(memory_space=pltpu.HBM),
            pl.BlockSpec(memory_space=pltpu.HBM),
            pl.BlockSpec(memory_space=pltpu.HBM),
        ],
        out_specs=(pl.BlockSpec(memory_space=pltpu.VMEM), pl.BlockSpec(memory_space=pltpu.VMEM)),
        scratch_shapes=[
            pltpu.VMEM((CORES, n_docs, width), train_docs.dtype),
            pltpu.VMEM((PARTS, X, Z, Y, own // PARTS, width), eval_rows.dtype),
            pltpu.VMEM((X, C, 1, own), jnp.int32),
            pltpu.VMEM((CORES, n_docs, LANES), f32),
            pltpu.VMEM((CORES, n_docs, LANES), f32),
            pltpu.VMEM((CORES, n_docs // LANES, LANES), f32),
            pltpu.VMEM((n_docs // LANES, LANES), f32),
            pltpu.VMEM((NBENCH, LANES), f32),
            pltpu.VMEM((C, 1, NBENCH), f32),
            pltpu.VMEM((R, 1, NBENCH), f32),
            pltpu.SemaphoreType.DMA((PARTS + 2,)),
            pltpu.SemaphoreType.DMA((copies,)),
            pltpu.SemaphoreType.DMA((copies,)),
        ],
        compiler_params=pltpu.CompilerParams(
            collective_id=0, has_side_effects=True, vmem_limit_bytes=48 * 1024 * 1024
        ),
    )(train_docs, eval_rows, bench_ids.reshape(1, own))
    return row_best.reshape(n_docs), bench_best.reshape(NBENCH)


def solution(mesh):
    columns = mesh.shape["col"]
    Y = split_col(columns)
    dims = (mesh.shape["row"] // CORES, columns // Y, Y)
    in_specs = (P(("row", "col"), None), P(("row", "col"), None), P(("row", "col"), None))
    out_specs = (P(("row", "col")), P())
    return jax.shard_map(
        functools.partial(body, dims), mesh=mesh, in_specs=in_specs, out_specs=out_specs, check_vma=False
    )
```
